32 devices in a mesh: groups: 2 (over y), blk: 16 (over z, x, core).
Axes of the slice: x: 2, y: 2, z: 4, core: 2. Of those that a mesh axis runs over, the one named last changes fastest.
Arguments:
- current_states: float32 [16, 8192], P(None, ('groups', 'blk')), parts along dimension 1, may hold values from -0.5 to 0.5
- next_states: float32 [16, 8192], P(None, ('groups', 'blk')), parts along dimension 1, may hold values from -1 to 1
- next_values: float32 [8192], P(('groups', 'blk')), parts along dimension 0, may hold values from 0 to 2.5
- vol_table: float32 [12, 16], replicated, may hold values from 0.15 to 0.45
- date_index: int32 [1], replicated, may hold values from 0 to 11
- strike: float32 [1], replicated, may hold values from 0.8 to 1.2
Outputs:
- continuation: float32 [8192], P(('groups', 'blk')), parts along dimension 0
- node_value: float32 [8192], P(('groups', 'blk')), parts along dimension 0
The draws below stay inside these ranges and needn't reach their ends.
There are 2 independent parts, one for each index of `groups`. The reference program is written for one: setup_inputs(seed, part) draws one part's arguments, and reference() takes and returns one part's arrays. A program takes and returns all parts, laid end to end along the dimension named above; an argument that names none is the same for every part. Nothing has to cross between parts.
All inputs are finite; a program needn't handle non-finite values.
Results may differ from the reference program's by a relative error of at most 0.00012.
Values sent between devices are 32-bit elements; how exact they have to be, the bound alone decides.
A program may use at most 64 MiB of HBM per device.

```python
import math
import jax
import jax.numpy as jnp
from jax import lax

ASSETS = 16
DATES = 12
NODES = 4096


def mesh_paths(key):
    folded = jax.random.fold_in(key, 7)
    key_list = jax.random.split(folded, 5)
    placing = (jnp.arange(NODES, dtype=jnp.float32) + 0.5) / NODES - 0.5
    heading = 0.05 * jnp.clip(jax.random.normal(key_list[0], (ASSETS,), jnp.float32), -2.0, 2.0)
    widths = jnp.exp(jax.random.uniform(key_list[1], (ASSETS,), jnp.float32, jnp.log(0.5), jnp.log(1.5)))
    jitter = jnp.clip(jax.random.normal(key_list[2], (ASSETS, NODES), jnp.float32), -4.0, 4.0)
    current = 0.03 * widths[:, None] * jitter + heading[:, None] * placing[None, :]
    moves = jnp.clip(jax.random.normal(key_list[3], (ASSETS, NODES), jnp.float32), -4.0, 4.0)
    following = current - 0.004 + 0.095 * moves
    extra = jnp.clip(jax.random.normal(key_list[4], (NODES,), jnp.float32), -4.0, 4.0)
    worth = jnp.maximum(jnp.max(jnp.exp(following), axis=0) - 1.0, 0.0) + 0.05 * jnp.exp(0.5 * extra)
    return (current, following, worth)


def draw_current_states(key, part):
    return mesh_paths(key)[0]


def draw_next_states(key, part):
    return mesh_paths(key)[1]


def draw_next_values(key, part):
    return mesh_paths(key)[2]


def setup_inputs(seed: int = 0, part: int = 0) -> dict:
    keys = jax.random.split(jax.random.key(seed), 7)
    own_keys = jax.random.split(jax.random.fold_in(keys[6], part), 7)
    return {
        "current_states": draw_current_states(jax.random.fold_in(jax.random.fold_in(keys[6], part), 71), part),
        "next_states": draw_next_states(jax.random.fold_in(jax.random.fold_in(keys[6], part), 71), part),
        "next_values": draw_next_values(jax.random.fold_in(jax.random.fold_in(keys[6], part), 71), part),
        "vol_table": jnp.clip(jnp.exp(jax.random.uniform(keys[3], (DATES, ASSETS), jnp.float32, math.log(0.15), math.log(0.45))), 0.15, 0.45),
        "date_index": jax.random.randint(keys[4], (1,), 0, DATES).astype(jnp.int32),
        "strike": jnp.clip(jax.random.uniform(keys[5], (1,), jnp.float32, 0.8, 1.2), 0.8, 1.2),
    }


rate_year = 0.05
step_years = 0.1

def scaled_states(current_states, next_states, vol_table, date_index):
    date_count = vol_table.shape[0]
    picked = (jnp.arange(date_count, dtype=jnp.int32) == date_index[0]).astype(jnp.float32)
    vol_row = lax.optimization_barrier(jnp.sum(vol_table * picked[:, None], axis=0))
    spread = vol_row * math.sqrt(step_years)
    drift_term = (rate_year - 0.5 * vol_row * vol_row) * step_years
    anchor = (current_states + drift_term[:, None]) / spread[:, None]
    target = next_states / spread[:, None]
    anchor_half = 0.5 * lax.optimization_barrier(jnp.sum(anchor * anchor, axis=0, keepdims=True))
    target_half = 0.5 * lax.optimization_barrier(jnp.sum(target * target, axis=0, keepdims=True))
    return (anchor, anchor_half, target, target_half)

def kernel_block(source_states, source_norms, sink_states, sink_norms):
    inner_term = lax.dot_general(source_states, sink_states, (((0,), (0,)), ((), ())), precision=lax.Precision.HIGHEST, preferred_element_type=jnp.float32)
    return jnp.exp(inner_term - source_norms.reshape(-1, 1) - sink_norms.reshape(1, -1))

def finish(current_states, totals, strike):
    continuation = math.exp(-rate_year * step_years) * totals[0] / totals[1]
    payoff = jnp.maximum(lax.optimization_barrier(jnp.max(jnp.exp(current_states), axis=0)) - strike[0], 0.0)
    return (continuation, jnp.maximum(payoff, continuation))

def reference(current_states, next_states, next_values, vol_table, date_index, strike):
    anchor, anchor_half, target, target_half = scaled_states(current_states, next_states, vol_table, date_index)
    node_count = anchor.shape[1]
    block_size = math.gcd(node_count, 1024)
    blocks = node_count // block_size

    def density_block(number):
        sink_part = lax.dynamic_slice_in_dim(target, number * block_size, block_size, 1)
        norm_part = lax.dynamic_slice_in_dim(target_half, number * block_size, block_size, 1)
        return lax.optimization_barrier(jnp.sum(kernel_block(sink_part, norm_part, anchor, anchor_half), axis=1))
    density = lax.map(density_block, jnp.arange(blocks, dtype=jnp.int32)).reshape(-1)
    ratios = jnp.stack([next_values / density, 1.0 / density], axis=0)

    def weighted_block(number):
        anchor_part = lax.dynamic_slice_in_dim(anchor, number * block_size, block_size, 1)
        half_part = lax.dynamic_slice_in_dim(anchor_half, number * block_size, block_size, 1)
        weights = kernel_block(target, target_half, anchor_part, half_part)
        return jnp.dot(ratios, weights, precision=lax.Precision.HIGHEST, preferred_element_type=jnp.float32)
    totals = lax.map(weighted_block, jnp.arange(blocks, dtype=jnp.int32))
    totals = jnp.transpose(totals, (1, 0, 2)).reshape(2, -1)
    return finish(current_states, totals, strike)
```

```python
import functools
import math

import jax
import jax.numpy as jnp
from jax import lax
from jax.experimental import pallas as pl
from jax.experimental.pallas import tpu as pltpu
from jax.sharding import PartitionSpec as P

rate_year = 0.05
step_years = 0.1
MESH = pl.DeviceIdType.MESH


def inner_size(count):
    size = 1
    while count % (2 * size) == 0 and (2 * size) ** 2 <= count:
        size *= 2
    return size


def split3(x):
    high = x.astype(jnp.bfloat16)
    rest = x - high.astype(jnp.float32)
    mid = rest.astype(jnp.bfloat16)
    low = (rest - mid.astype(jnp.float32)).astype(jnp.bfloat16)
    return high, mid, low


def norm_rows(x, first):
    norm = -0.5 * jnp.sum(x * x, axis=0, keepdims=True)
    pieces = [piece.astype(jnp.float32) for piece in split3(norm)]
    row = lax.broadcasted_iota(jnp.int32, (16, x.shape[1]), 0)
    at = 0 if first else 3
    rows = jnp.where((row >= 3 - at) & (row < 6 - at), 1.0, 0.0)
    for number, piece in enumerate(pieces):
        rows = jnp.where(row == at + number, piece, rows)
    return rows.astype(jnp.bfloat16)


def anchor_stack(x):
    high, mid, low = split3(x)
    zero = jnp.zeros_like(high)
    return jnp.concatenate([high, high, high, mid, mid, low, norm_rows(x, True), zero], axis=0)


def target_stack(x):
    high, mid, low = split3(x)
    zero = jnp.zeros_like(high)
    return jnp.concatenate([high, mid, low, high, mid, high, norm_rows(x, False), zero], axis=0)


def kernel(
    inner_count,
    outer_count,
    cur_hbm,
    next_hbm,
    val_hbm,
    vol_hbm,
    date_hbm,
    strike_hbm,
    out_ref,
    anc,
    tgt,
    val,
    vol,
    date,
    strike,
    kmat,
    tstack,
    dens_own,
    dens_in,
    part_own,
    part_in,
    in_sem,
    anc_send,
    anc_recv,
    tgt_send,
    tgt_recv,
    val_send,
    val_recv,
    dens_send,
    dens_recv,
    part_send,
    part_recv,
):
    g, h = inner_count, outer_count
    n = anc.shape[2]
    me = lax.axis_index("blk")
    inner, outer = lax.rem(me, g), lax.div(me, g)

    def inner_peer(s):
        return {"blk": outer * g + lax.rem(inner + s, g)}

    def outer_peer(s):
        return {"blk": lax.rem(outer + s, h) * g + inner}

    barrier = pltpu.get_barrier_semaphore()
    for s in range(1, h):
        pl.semaphore_signal(barrier, inc=1, device_id=outer_peer(s), device_id_type=MESH)
    for s in range(1, g):
        pl.semaphore_signal(barrier, inc=1, device_id=inner_peer(s), device_id_type=MESH)

    loads = [
        pltpu.make_async_copy(src, dst, in_sem.at[number])
        for number, (src, dst) in enumerate(
            [
                (cur_hbm, anc.at[0]),
                (next_hbm, tgt.at[inner]),
                (val_hbm, val.at[inner]),
                (vol_hbm, vol),
                (date_hbm, date),
                (strike_hbm, strike),
            ]
        )
    ]
    for load in loads:
        load.start()
    for load in loads:
        load.wait()

    dates, assets = vol.shape
    picked = lax.broadcasted_iota(jnp.int32, (dates, assets), 0) == date[0]
    vol_lanes = jnp.sum(jnp.where(picked, vol[...], 0.0), axis=0, keepdims=True)
    eye = lax.broadcasted_iota(jnp.int32, (assets, assets), 0) == lax.broadcasted_iota(
        jnp.int32, (assets, assets), 1
    )
    vol_row = jnp.sum(jnp.where(eye, vol_lanes, 0.0), axis=1, keepdims=True)
    scale = math.sqrt(math.log2(math.e)) / (vol_row * math.sqrt(step_years))
    drift = (rate_year - 0.5 * vol_row * vol_row) * step_years

    pl.semaphore_wait(barrier, (h - 1) + (g - 1))

    anc_copies, tgt_copies, val_copies = {}, {}, {}
    far_first = sorted(range(1, h), key=lambda s: -min(s, h - s))
    for s in far_first:
        anc_copies[s] = pltpu.make_async_remote_copy(
            src_ref=anc.at[0],
            dst_ref=anc.at[s],
            send_sem=anc_send.at[s],
            recv_sem=anc_recv.at[s],
            device_id=outer_peer(s),
            device_id_type=MESH,
        )
        anc_copies[s].start()
    for s in range(1, g):
        tgt_copies[s] = pltpu.make_async_remote_copy(
            src_ref=tgt.at[inner],
            dst_ref=tgt.at[inner],
            send_sem=tgt_send.at[s],
            recv_sem=tgt_recv.at[s],
            device_id=inner_peer(s),
            device_id_type=MESH,
        )
        tgt_copies[s].start()
    for s in range(1, g):
        val_copies[s] = pltpu.make_async_remote_copy(
            src_ref=val.at[inner],
            dst_ref=val.at[inner],
            send_sem=val_send.at[s],
            recv_sem=val_recv.at[s],
            device_id=inner_peer(s),
            device_id_type=MESH,
        )
        val_copies[s].start()

    def anchor_rows(s):
        stack = anchor_stack((anc[s] + drift) * scale)
        return jnp.transpose(stack)

    own_rows = anchor_rows(0)
    for s in range(1, g):
        tgt_copies[s].wait_recv()
    for q in range(g):
        tstack[:, q * n : (q + 1) * n] = target_stack(tgt[q] * scale)

    density = jnp.zeros((8, g * n), jnp.float32)
    for s in [0] + far_first[::-1]:
        if s:
            anc_copies[s].wait_recv()
            rows = anchor_rows(s)
        else:
            rows = own_rows
        exponent = jnp.dot(rows, tstack[...], preferred_element_type=jnp.float32)
        block = jnp.exp2(exponent)
        kmat[s] = block
        density = density + jnp.sum(block.reshape(n // 8, 8, g * n), axis=0)

    dens_own[...] = jnp.sum(density, axis=0, keepdims=True)
    dens_copies = {}
    for s in range(1, g):
        dens_copies[s] = pltpu.make_async_remote_copy(
            src_ref=dens_own,
            dst_ref=dens_in.at[s],
            send_sem=dens_send.at[s],
            recv_sem=dens_recv.at[s],
            device_id=inner_peer(s),
            device_id_type=MESH,
        )
        dens_copies[s].start()
    payoff = jnp.maximum(
        jnp.max(jnp.exp(anc[0]), axis=0, keepdims=True) - strike[0], 0.0
    )
    for s in range(1, g):
        val_copies[s].wait_recv()
    total = dens_own[...]
    for s in range(1, g):
        dens_copies[s].wait_recv()
        total = total + dens_in[s]
    inverse = 1.0 / total
    values = jnp.concatenate([val[q] for q in range(g)], axis=1)
    worth = values / total

    part_copies = {}
    for s in far_first + [0]:
        weighted = jnp.zeros((n, 128), jnp.float32)
        mass = jnp.zeros((n, 128), jnp.float32)
        for q in range(g * n // 128):
            tile = kmat[s, :, q * 128 : (q + 1) * 128]
            weighted = weighted + tile * worth[:, q * 128 : (q + 1) * 128]
            mass = mass + tile * inverse[:, q * 128 : (q + 1) * 128]
        part_own[s, 0:1, :] = jnp.sum(jnp.transpose(weighted), axis=0, keepdims=True)
        part_own[s, 1:2, :] = jnp.sum(jnp.transpose(mass), axis=0, keepdims=True)
        if s:
            part_copies[s] = pltpu.make_async_remote_copy(
                src_ref=part_own.at[s],
                dst_ref=part_in.at[s],
                send_sem=part_send.at[s],
                recv_sem=part_recv.at[s],
                device_id=outer_peer(h - s),
                device_id_type=MESH,
            )
            part_copies[s].start()
    sums = part_own[0]
    for s in far_first[::-1]:
        part_copies[s].wait_recv()
        sums = sums + part_in[s]
    out_ref[0:2, :] = sums
    out_ref[2:3, :] = payoff
    for copies in (anc_copies, tgt_copies, val_copies, dens_copies, part_copies):
        for copy in copies.values():
            copy.wait_send()


def body(count, current_states, next_states, next_values, vol_table, date_index, strike):
    assets, n = current_states.shape
    g = inner_size(count)
    h = count // g
    f32 = jnp.float32
    dma = pltpu.SemaphoreType.DMA
    sums = pl.pallas_call(
        functools.partial(kernel, g, h),
        out_shape=jax.ShapeDtypeStruct((3, n), f32),
        in_specs=[pl.BlockSpec(memory_space=pl.ANY)] * 6,
        out_specs=pl.BlockSpec(memory_space=pltpu.VMEM),
        scratch_shapes=[
            pltpu.VMEM((h, assets, n), f32),
            pltpu.VMEM((g, assets, n), f32),
            pltpu.VMEM((g, 1, n), f32),
            pltpu.VMEM(vol_table.shape, f32),
            pltpu.SMEM((1,), jnp.int32),
            pltpu.SMEM((1,), f32),
            pltpu.VMEM((h, n, g * n), f32),
            pltpu.VMEM((128, g * n), jnp.bfloat16),
            pltpu.VMEM((1, g * n), f32),
            pltpu.VMEM((g, 1, g * n), f32),
            pltpu.VMEM((h, 2, n), f32),
            pltpu.VMEM((h, 2, n), f32),
            dma((6,)),
            dma((h,)),
            dma((h,)),
            dma((g,)),
            dma((g,)),
            dma((g,)),
            dma((g,)),
            dma((g,)),
            dma((g,)),
            dma((h,)),
            dma((h,)),
        ],
        compiler_params=pltpu.CompilerParams(collective_id=0, has_side_effects=True),
    )(current_states, next_states, next_values.reshape(1, n), vol_table, date_index, strike)
    continuation = math.exp(-rate_year * step_years) * sums[0] / sums[1]
    return (continuation, jnp.maximum(sums[2], continuation))


def solution(mesh):
    placed = (
        P(None, ("groups", "blk")),
        P(None, ("groups", "blk")),
        P(("groups", "blk")),
        P(),
        P(),
        P(),
    )
    return jax.shard_map(
        functools.partial(body, mesh.shape["blk"]),
        mesh=mesh,
        in_specs=placed,
        out_specs=(P(("groups", "blk")), P(("groups", "blk"))),
        check_vma=False,
    )
```

```python
import functools
import math

import jax
import jax.numpy as jnp
from jax import lax
from jax.experimental import pallas as pl
from jax.experimental.pallas import tpu as pltpu
from jax.sharding import PartitionSpec as P

rate_year = 0.05
step_years = 0.1
MESH = pl.DeviceIdType.MESH


def inner_size(count):
    size = 1
    while count % (2 * size) == 0 and (2 * size) ** 2 <= count:
        size *= 2
    return size


def radices(size):
    digits = size.bit_length() - 1
    return (2,) * digits if 2**digits == size else (size,)


def moved(place, offset, size, sign):
    result, unit = 0, 1
    for radix in radices(size):
        digit = (place // unit + sign * (offset // unit % radix) + radix) % radix
        result = result + digit * unit
        unit *= radix
    return result


def digit_count(offset):
    return bin(offset).count("1")


def split3(x):
    high = x.astype(jnp.bfloat16)
    rest = x - high.astype(jnp.float32)
    mid = rest.astype(jnp.bfloat16)
    low = (rest - mid.astype(jnp.float32)).astype(jnp.bfloat16)
    return high, mid, low


def norm_rows(x, first):
    norm = -0.5 * jnp.sum(x * x, axis=0, keepdims=True)
    pieces = [piece.astype(jnp.float32) for piece in split3(norm)]
    row = lax.broadcasted_iota(jnp.int32, (16, x.shape[1]), 0)
    at = 0 if first else 3
    rows = jnp.where((row >= 3 - at) & (row < 6 - at), 1.0, 0.0)
    for number, piece in enumerate(pieces):
        rows = jnp.where(row == at + number, piece, rows)
    return rows.astype(jnp.bfloat16)


def anchor_stack(x):
    high, mid, low = split3(x)
    zero = jnp.zeros_like(high)
    return jnp.concatenate([high, high, high, mid, mid, low, norm_rows(x, True), zero], axis=0)


def target_stack(x):
    high, mid, low = split3(x)
    zero = jnp.zeros_like(high)
    return jnp.concatenate([high, mid, low, high, mid, high, norm_rows(x, False), zero], axis=0)


def kernel(
    inner_count,
    outer_count,
    cur_hbm,
    next_hbm,
    val_hbm,
    vol_hbm,
    date_hbm,
    strike_hbm,
    cont_ref,
    node_ref,
    anc,
    tgt,
    val,
    vol,
    date,
    strike,
    kmat,
    dens_own,
    dens_in,
    part_own,
    part_in,
    in_sem,
    anc_send,
    anc_recv,
    tgt_send,
    tgt_recv,
    val_send,
    val_recv,
    dens_send,
    dens_recv,
    part_send,
    part_recv,
):
    g, h = inner_count, outer_count
    n = anc.shape[2]
    low_count = min(g, 2)
    me = lax.axis_index("blk")
    low = me % low_count
    outer = me // low_count % h
    inner = me // (low_count * h) * low_count + low

    def place(inner_place, outer_place):
        high = inner_place // low_count
        return {"blk": (high * h + outer_place) * low_count + inner_place % low_count}

    def inner_peer(q):
        return place(moved(inner, q, g, 1), outer)

    def outer_peer(s, sign=1):
        return place(inner, moved(outer, s, h, sign))

    def owner(q):
        return moved(inner, q, g, -1)

    inner_offsets = list(range(g - 1, 0, -1))
    outer_offsets = sorted(range(1, h), key=lambda s: (-digit_count(s), -s))

    barrier = pltpu.get_barrier_semaphore()
    for q in inner_offsets:
        pl.semaphore_signal(barrier, inc=1, device_id=inner_peer(q), device_id_type=MESH)
    for s in outer_offsets:
        pl.semaphore_signal(barrier, inc=1, device_id=outer_peer(s), device_id_type=MESH)

    loads = [
        pltpu.make_async_copy(src, dst, in_sem.at[number])
        for number, (src, dst) in enumerate(
            [
                (next_hbm, tgt.at[inner]),
                (cur_hbm, anc.at[0]),
                (vol_hbm, vol),
                (date_hbm, date),
                (val_hbm, val.at[inner]),
                (strike_hbm, strike),
            ]
        )
    ]
    for load in loads:
        load.start()

    def inner_copies(ref, dst, send, recv):
        return {
            q: pltpu.make_async_remote_copy(
                src_ref=ref,
                dst_ref=dst(q),
                send_sem=send.at[q],
                recv_sem=recv.at[q],
                device_id=inner_peer(q),
                device_id_type=MESH,
            )
            for q in inner_offsets
        }

    tgt_copies = inner_copies(tgt.at[inner], lambda q: tgt.at[inner], tgt_send, tgt_recv)
    val_copies = inner_copies(val.at[inner], lambda q: val.at[inner], val_send, val_recv)
    dens_copies = inner_copies(dens_own, lambda q: dens_in.at[q], dens_send, dens_recv)
    anc_copies = {
        s: pltpu.make_async_remote_copy(
            src_ref=anc.at[0],
            dst_ref=anc.at[s],
            send_sem=anc_send.at[s],
            recv_sem=anc_recv.at[s],
            device_id=outer_peer(s),
            device_id_type=MESH,
        )
        for s in outer_offsets
    }
    part_copies = {
        s: pltpu.make_async_remote_copy(
            src_ref=part_own.at[s],
            dst_ref=part_in.at[s],
            send_sem=part_send.at[s],
            recv_sem=part_recv.at[s],
            device_id=outer_peer(s, -1),
            device_id_type=MESH,
        )
        for s in outer_offsets
    }

    pl.semaphore_wait(barrier, (h - 1) + (g - 1))
    loads[0].wait()
    for q in inner_offsets:
        tgt_copies[q].start()
    loads[1].wait()
    for s in outer_offsets:
        anc_copies[s].start()
    for load in loads[2:]:
        load.wait()
    for q in inner_offsets:
        val_copies[q].start()

    dates, assets = vol.shape
    picked = lax.broadcasted_iota(jnp.int32, (dates, assets), 0) == date[0]
    vol_lanes = jnp.sum(jnp.where(picked, vol[...], 0.0), axis=0, keepdims=True)
    eye = lax.broadcasted_iota(jnp.int32, (assets, assets), 0) == lax.broadcasted_iota(
        jnp.int32, (assets, assets), 1
    )
    vol_row = jnp.sum(jnp.where(eye, vol_lanes, 0.0), axis=1, keepdims=True)
    scale = math.sqrt(math.log2(math.e)) / (vol_row * math.sqrt(step_years))
    drift = (rate_year - 0.5 * vol_row * vol_row) * step_years

    rows, columns = {}, {}
    outer_order = [0] + outer_offsets[::-1]
    near = [q for q in range(g) if q < low_count]
    far = [q for q in range(g) if q >= low_count]

    def block(s, q):
        exponent = jnp.dot(rows[s], columns[q], preferred_element_type=jnp.float32)
        weights = jnp.exp2(exponent)
        kmat[s, :, q * n : (q + 1) * n] = weights
        return jnp.sum(weights.reshape(n // 8, 8, n), axis=0)

    density = {q: jnp.zeros((8, n), jnp.float32) for q in range(g)}
    for part in (near, far):
        for q in part:
            if q:
                tgt_copies[q].wait_recv()
            columns[q] = target_stack(tgt[owner(q)] * scale)
        for s in outer_order:
            if s not in rows:
                if s:
                    anc_copies[s].wait_recv()
                rows[s] = jnp.transpose(anchor_stack((anc[s] + drift) * scale))
            for q in part:
                density[q] = density[q] + block(s, q)
        for q in part:
            dens_own[owner(q)] = jnp.sum(density[q], axis=0, keepdims=True)

    for q in inner_offsets:
        dens_copies[q].start()
    payoff = jnp.maximum(
        jnp.max(jnp.exp(anc[0]), axis=0, keepdims=True) - strike[0], 0.0
    )
    for q in inner_offsets:
        val_copies[q].wait_recv()
    for q in inner_offsets:
        dens_copies[q].wait_recv()
    worth, inverse = {}, {}
    for q in range(g):
        total = dens_own[owner(q)]
        for p in inner_offsets:
            total = total + dens_in[p, owner(q)]
        inverse[q] = 1.0 / total
        worth[q] = val[owner(q)] / total

    for s in outer_order[::-1]:
        weighted = jnp.zeros((n, 128), jnp.float32)
        mass = jnp.zeros((n, 128), jnp.float32)
        for q in range(g):
            for c in range(0, n, 128):
                tile = kmat[s, :, q * n + c : q * n + c + 128]
                weighted = weighted + tile * worth[q][:, c : c + 128]
                mass = mass + tile * inverse[q][:, c : c + 128]
        part_own[s, 0:1, :] = jnp.sum(jnp.transpose(weighted), axis=0, keepdims=True)
        part_own[s, 1:2, :] = jnp.sum(jnp.transpose(mass), axis=0, keepdims=True)
        if s:
            part_copies[s].start()
    sums = part_own[0]
    for s in outer_offsets[::-1]:
        part_copies[s].wait_recv()
        sums = sums + part_in[s]
    continuation = math.exp(-rate_year * step_years) * sums[0:1] / sums[1:2]
    cont_ref[...] = continuation
    node_ref[...] = jnp.maximum(payoff, continuation)
    for copies in (anc_copies, tgt_copies, val_copies, dens_copies, part_copies):
        for copy in copies.values():
            copy.wait_send()


def body(count, current_states, next_states, next_values, vol_table, date_index, strike):
    assets, n = current_states.shape
    g = inner_size(count)
    h = count // g
    f32 = jnp.float32
    dma = pltpu.SemaphoreType.DMA
    row = jax.ShapeDtypeStruct((1, n), f32)
    continuation, node_value = pl.pallas_call(
        functools.partial(kernel, g, h),
        out_shape=(row, row),
        in_specs=[pl.BlockSpec(memory_space=pltpu.HBM)] * 6,
        out_specs=(pl.BlockSpec(memory_space=pltpu.VMEM),) * 2,
        scratch_shapes=[
            pltpu.VMEM((h, assets, n), f32),
            pltpu.VMEM((g, assets, n), f32),
            pltpu.VMEM((g, 1, n), f32),
            pltpu.VMEM(vol_table.shape, f32),
            pltpu.SMEM((1,), jnp.int32),
            pltpu.SMEM((1,), f32),
            pltpu.VMEM((h, n, g * n), f32),
            pltpu.VMEM((g, 1, n), f32),
            pltpu.VMEM((g, g, 1, n), f32),
            pltpu.VMEM((h, 2, n), f32),
            pltpu.VMEM((h, 2, n), f32),
            dma((6,)),
            dma((h,)),
            dma((h,)),
            dma((g,)),
            dma((g,)),
            dma((g,)),
            dma((g,)),
            dma((g,)),
            dma((g,)),
            dma((h,)),
            dma((h,)),
        ],
        compiler_params=pltpu.CompilerParams(collective_id=0, has_side_effects=True),
    )(current_states, next_states, next_values.reshape(1, n), vol_table, date_index, strike)
    return (continuation.reshape(n), node_value.reshape(n))


def solution(mesh):
    placed = (
        P(None, ("groups", "blk")),
        P(None, ("groups", "blk")),
        P(("groups", "blk")),
        P(),
        P(),
        P(),
    )
    return jax.shard_map(
        functools.partial(body, mesh.shape["blk"]),
        mesh=mesh,
        in_specs=placed,
        out_specs=(P(("groups", "blk")), P(("groups", "blk"))),
        check_vma=False,
    )
```

```python
import functools
import math

import jax
import jax.numpy as jnp
from jax import lax
from jax.experimental import pallas as pl
from jax.experimental.pallas import tpu as pltpu
from jax.sharding import PartitionSpec as P

rate_year = 0.05
step_years = 0.1
MESH = pl.DeviceIdType.MESH


def inner_size(count):
    size = 1
    while count % (2 * size) == 0 and (2 * size) ** 2 <= count:
        size *= 2
    return size


def radices(size):
    digits = size.bit_length() - 1
    return (2,) * digits if 2**digits == size else (size,)


def moved(place, offset, size, sign):
    result, unit = 0, 1
    for radix in radices(size):
        digit = (place // unit + sign * (offset // unit % radix) + radix) % radix
        result = result + digit * unit
        unit *= radix
    return result


def digit_count(offset):
    return bin(offset).count("1")


def split3(x):
    high = x.astype(jnp.bfloat16)
    rest = x - high.astype(jnp.float32)
    mid = rest.astype(jnp.bfloat16)
    low = (rest - mid.astype(jnp.float32)).astype(jnp.bfloat16)
    return high, mid, low


def norm_rows(x, first):
    norm = -0.5 * jnp.sum(x * x, axis=0, keepdims=True)
    pieces = [piece.astype(jnp.float32) for piece in split3(norm)]
    row = lax.broadcasted_iota(jnp.int32, (16, x.shape[1]), 0)
    at = 0 if first else 3
    rows = jnp.where((row >= 3 - at) & (row < 6 - at), 1.0, 0.0)
    for number, piece in enumerate(pieces):
        rows = jnp.where(row == at + number, piece, rows)
    return rows.astype(jnp.bfloat16)


def anchor_stack(x):
    high, mid, low = split3(x)
    zero = jnp.zeros_like(high)
    return jnp.concatenate([high, high, high, mid, mid, low, norm_rows(x, True), zero], axis=0)


def target_stack(x):
    high, mid, low = split3(x)
    zero = jnp.zeros_like(high)
    return jnp.concatenate([high, mid, low, high, mid, high, norm_rows(x, False), zero], axis=0)


def kernel(
    inner_count,
    outer_count,
    cur_hbm,
    next_hbm,
    val_hbm,
    vol_hbm,
    date_hbm,
    strike_hbm,
    weighted_ref,
    mass_ref,
    payoff_ref,
    anc,
    tgt,
    val,
    vol,
    date,
    strike,
    kmat,
    dens_own,
    dens_in,
    part_own,
    part_in,
    in_sem,
    anc_send,
    anc_recv,
    tgt_send,
    tgt_recv,
    val_send,
    val_recv,
    dens_send,
    dens_recv,
    part_send,
    part_recv,
):
    g, h = inner_count, outer_count
    n = anc.shape[2]
    low_count = min(g, 2)
    me = lax.axis_index("blk")
    low = me % low_count
    outer = me // low_count % h
    inner = me // (low_count * h) * low_count + low

    def place(inner_place, outer_place):
        high = inner_place // low_count
        return {"blk": (high * h + outer_place) * low_count + inner_place % low_count}

    def inner_peer(q):
        return place(moved(inner, q, g, 1), outer)

    def outer_peer(s, sign=1):
        return place(inner, moved(outer, s, h, sign))

    def owner(q):
        return moved(inner, q, g, -1)

    inner_offsets = list(range(g - 1, 0, -1))
    outer_offsets = sorted(range(1, h), key=lambda s: (-digit_count(s), -s))

    barrier = pltpu.get_barrier_semaphore()
    for q in inner_offsets:
        pl.semaphore_signal(barrier, inc=1, device_id=inner_peer(q), device_id_type=MESH)
    for s in outer_offsets:
        pl.semaphore_signal(barrier, inc=1, device_id=outer_peer(s), device_id_type=MESH)

    loads = [
        pltpu.make_async_copy(src, dst, in_sem.at[number])
        for number, (src, dst) in enumerate(
            [
                (next_hbm, tgt.at[inner]),
                (cur_hbm, anc.at[0]),
                (vol_hbm, vol),
                (date_hbm, date),
                (val_hbm, val.at[inner]),
                (strike_hbm, strike),
            ]
        )
    ]
    for load in loads:
        load.start()

    def inner_copies(ref, dst, send, recv):
        return {
            q: pltpu.make_async_remote_copy(
                src_ref=ref,
                dst_ref=dst(q),
                send_sem=send.at[q],
                recv_sem=recv.at[q],
                device_id=inner_peer(q),
                device_id_type=MESH,
            )
            for q in inner_offsets
        }

    tgt_copies = inner_copies(tgt.at[inner], lambda q: tgt.at[inner], tgt_send, tgt_recv)
    val_copies = inner_copies(val.at[inner], lambda q: val.at[inner], val_send, val_recv)
    dens_copies = inner_copies(dens_own, lambda q: dens_in.at[q], dens_send, dens_recv)
    anc_copies = {
        s: pltpu.make_async_remote_copy(
            src_ref=anc.at[0],
            dst_ref=anc.at[s],
            send_sem=anc_send.at[s],
            recv_sem=anc_recv.at[s],
            device_id=outer_peer(s),
            device_id_type=MESH,
        )
        for s in outer_offsets
    }
    part_copies = {
        s: pltpu.make_async_remote_copy(
            src_ref=part_own.at[s],
            dst_ref=part_in.at[s],
            send_sem=part_send.at[s],
            recv_sem=part_recv.at[s],
            device_id=outer_peer(s, -1),
            device_id_type=MESH,
        )
        for s in outer_offsets
    }

    pl.semaphore_wait(barrier, (h - 1) + (g - 1))
    loads[0].wait()
    for q in inner_offsets:
        tgt_copies[q].start()
    loads[1].wait()
    for s in outer_offsets:
        anc_copies[s].start()
    for load in loads[2:]:
        load.wait()
    for q in inner_offsets:
        val_copies[q].start()

    dates, assets = vol.shape
    picked = lax.broadcasted_iota(jnp.int32, (dates, assets), 0) == date[0]
    vol_lanes = jnp.sum(jnp.where(picked, vol[...], 0.0), axis=0, keepdims=True)
    eye = lax.broadcasted_iota(jnp.int32, (assets, assets), 0) == lax.broadcasted_iota(
        jnp.int32, (assets, assets), 1
    )
    vol_row = jnp.sum(jnp.where(eye, vol_lanes, 0.0), axis=1, keepdims=True)
    scale = math.sqrt(math.log2(math.e)) / (vol_row * math.sqrt(step_years))
    drift = (rate_year - 0.5 * vol_row * vol_row) * step_years

    rows, columns = {}, {}
    outer_order = [0] + outer_offsets[::-1]
    near = [q for q in range(g) if q < low_count]
    far = [q for q in range(g) if q >= low_count]

    def block(s, q):
        exponent = jnp.dot(rows[s], columns[q], preferred_element_type=jnp.float32)
        weights = jnp.exp2(exponent)
        kmat[s, :, q * n : (q + 1) * n] = weights
        return jnp.sum(weights.reshape(n // 8, 8, n), axis=0)

    density = {q: jnp.zeros((8, n), jnp.float32) for q in range(g)}
    for part in (near, far):
        for q in part:
            if q:
                tgt_copies[q].wait_recv()
            columns[q] = target_stack(tgt[owner(q)] * scale)
        for s in outer_order:
            if s not in rows:
                if s:
                    anc_copies[s].wait_recv()
                rows[s] = jnp.transpose(anchor_stack((anc[s] + drift) * scale))
            for q in part:
                density[q] = density[q] + block(s, q)
        for q in part:
            dens_own[owner(q)] = jnp.sum(density[q], axis=0, keepdims=True)

    for q in inner_offsets:
        dens_copies[q].start()
    payoff = jnp.maximum(
        jnp.max(jnp.exp(anc[0]), axis=0, keepdims=True) - strike[0], 0.0
    )
    for q in inner_offsets:
        val_copies[q].wait_recv()
    for q in inner_offsets:
        dens_copies[q].wait_recv()
    worth, inverse = {}, {}
    for q in range(g):
        total = dens_own[owner(q)]
        for p in inner_offsets:
            total = total + dens_in[p, owner(q)]
        inverse[q] = 1.0 / total
        worth[q] = val[owner(q)] / total

    for s in outer_order[::-1]:
        weighted = jnp.zeros((n, 128), jnp.float32)
        mass = jnp.zeros((n, 128), jnp.float32)
        for q in range(g):
            for c in range(0, n, 128):
                tile = kmat[s, :, q * n + c : q * n + c + 128]
                weighted = weighted + tile * worth[q][:, c : c + 128]
                mass = mass + tile * inverse[q][:, c : c + 128]
        part_own[s, 0:1, :] = jnp.sum(jnp.transpose(weighted), axis=0, keepdims=True)
        part_own[s, 1:2, :] = jnp.sum(jnp.transpose(mass), axis=0, keepdims=True)
        if s:
            part_copies[s].start()
    sums = part_own[0]
    for s in outer_offsets[::-1]:
        part_copies[s].wait_recv()
        sums = sums + part_in[s]
    weighted_ref[...] = sums[0]
    mass_ref[...] = sums[1]
    payoff_ref[...] = payoff.reshape(n)
    for copies in (anc_copies, tgt_copies, val_copies, dens_copies, part_copies):
        for copy in copies.values():
            copy.wait_send()


def body(count, current_states, next_states, next_values, vol_table, date_index, strike):
    assets, n = current_states.shape
    g = inner_size(count)
    h = count // g
    f32 = jnp.float32
    dma = pltpu.SemaphoreType.DMA
    row = pltpu.VMEM((n,), f32)
    w, m, p = pl.pallas_call(
        functools.partial(kernel, g, h),
        out_shape=(row, row, row),
        in_specs=[pl.BlockSpec(memory_space=pltpu.HBM)] * 6,
        out_specs=(pl.BlockSpec(memory_space=pltpu.VMEM),) * 3,
        scratch_shapes=[
            pltpu.VMEM((h, assets, n), f32),
            pltpu.VMEM((g, assets, n), f32),
            pltpu.VMEM((g, 1, n), f32),
            pltpu.VMEM(vol_table.shape, f32),
            pltpu.SMEM((1,), jnp.int32),
            pltpu.SMEM((1,), f32),
            pltpu.VMEM((h, n, g * n), f32),
            pltpu.VMEM((g, 1, n), f32),
            pltpu.VMEM((g, g, 1, n), f32),
            pltpu.VMEM((h, 2, n), f32),
            pltpu.VMEM((h, 2, n), f32),
            dma((6,)),
            dma((h,)),
            dma((h,)),
            dma((g,)),
            dma((g,)),
            dma((g,)),
            dma((g,)),
            dma((g,)),
            dma((g,)),
            dma((h,)),
            dma((h,)),
        ],
        compiler_params=pltpu.CompilerParams(collective_id=0, has_side_effects=True),
    )(current_states, next_states, next_values.reshape(1, n), vol_table, date_index, strike)
    c = math.exp(-rate_year * step_years) * w / m
    return (c, jnp.maximum(p, c))


def solution(mesh):
    placed = (
        P(None, ("groups", "blk")),
        P(None, ("groups", "blk")),
        P(("groups", "blk")),
        P(),
        P(),
        P(),
    )
    return jax.shard_map(
        functools.partial(body, mesh.shape["blk"]),
        mesh=mesh,
        in_specs=placed,
        out_specs=(P(("groups", "blk")), P(("groups", "blk"))),
        check_vma=False,
    )
```

```python
import functools
import math

import jax
import jax.numpy as jnp
from jax import lax
from jax.experimental import pallas as pl
from jax.experimental.pallas import tpu as pltpu
from jax.sharding import PartitionSpec as P

rate_year = 0.05
step_years = 0.1
MESH = pl.DeviceIdType.MESH


def inner_size(count):
    size = 1
    while count % (2 * size) == 0 and (2 * size) ** 2 <= count:
        size *= 2
    return size


def radices(size):
    digits = size.bit_length() - 1
    return (2,) * digits if 2**digits == size else (size,)


def moved(place, offset, size, sign):
    result, unit = 0, 1
    for radix in radices(size):
        digit = (place // unit + sign * (offset // unit % radix) + radix) % radix
        result = result + digit * unit
        unit *= radix
    return result


def digit_count(offset):
    return bin(offset).count("1")


def split3(x):
    high = x.astype(jnp.bfloat16)
    rest = x - high.astype(jnp.float32)
    mid = rest.astype(jnp.bfloat16)
    low = (rest - mid.astype(jnp.float32)).astype(jnp.bfloat16)
    return high, mid, low


def norm_rows(x, first):
    norm = -0.5 * jnp.sum(x * x, axis=0, keepdims=True)
    pieces = [piece.astype(jnp.float32) for piece in split3(norm)]
    row = lax.broadcasted_iota(jnp.int32, (16, x.shape[1]), 0)
    at = 0 if first else 3
    rows = jnp.where((row >= 3 - at) & (row < 6 - at), 1.0, 0.0)
    for number, piece in enumerate(pieces):
        rows = jnp.where(row == at + number, piece, rows)
    return rows.astype(jnp.bfloat16)


def anchor_stack(x):
    high, mid, low = split3(x)
    zero = jnp.zeros_like(high)
    return jnp.concatenate([high, high, high, mid, mid, low, norm_rows(x, True), zero], axis=0)


def target_stack(x):
    high, mid, low = split3(x)
    zero = jnp.zeros_like(high)
    return jnp.concatenate([high, mid, low, high, mid, high, norm_rows(x, False), zero], axis=0)


def kernel(
    inner_count,
    outer_count,
    cur_hbm,
    next_hbm,
    val_hbm,
    vol_hbm,
    date_hbm,
    weighted_ref,
    mass_ref,
    best_ref,
    anc,
    tgt,
    val,
    vol,
    date,
    kmat,
    dens_own,
    dens_in,
    part_own,
    part_in,
    in_sem,
    anc_send,
    anc_recv,
    tgt_send,
    tgt_recv,
    val_send,
    val_recv,
    dens_send,
    dens_recv,
    part_send,
    part_recv,
):
    g, h = inner_count, outer_count
    n = anc.shape[2]
    low_count = min(g, 2)
    me = lax.axis_index("blk")
    outer = me // low_count % h
    low = (me + outer * 2 // h) % low_count
    inner = me // (low_count * h) * low_count + low

    def place(inner_place, outer_place):
        high = inner_place // low_count
        turned = (inner_place + outer_place * 2 // h) % low_count
        return {"blk": (high * h + outer_place) * low_count + turned}

    def inner_peer(q):
        return place(moved(inner, q, g, 1), outer)

    def outer_peer(s, sign=1):
        return place(inner, moved(outer, s, h, sign))

    def owner(q):
        return moved(inner, q, g, -1)

    inner_offsets = list(range(g - 1, 0, -1))
    outer_offsets = sorted(range(1, h), key=lambda s: (-digit_count(s), -s))

    barrier = pltpu.get_barrier_semaphore()
    for q in inner_offsets:
        pl.semaphore_signal(barrier, inc=1, device_id=inner_peer(q), device_id_type=MESH)
    for s in outer_offsets:
        pl.semaphore_signal(barrier, inc=1, device_id=outer_peer(s), device_id_type=MESH)

    loads = [
        pltpu.make_async_copy(src, dst, in_sem.at[number])
        for number, (src, dst) in enumerate(
            [
                (next_hbm, tgt.at[inner]),
                (cur_hbm, anc.at[0]),
                (vol_hbm, vol),
                (date_hbm, date),
                (val_hbm, val.at[inner]),
            ]
        )
    ]
    for load in loads:
        load.start()

    def inner_copies(ref, dst, send, recv):
        return {
            q: pltpu.make_async_remote_copy(
                src_ref=ref,
                dst_ref=dst(q),
                send_sem=send.at[q],
                recv_sem=recv.at[q],
                device_id=inner_peer(q),
                device_id_type=MESH,
            )
            for q in inner_offsets
        }

    tgt_copies = inner_copies(tgt.at[inner], lambda q: tgt.at[inner], tgt_send, tgt_recv)
    val_copies = inner_copies(val.at[inner], lambda q: val.at[inner], val_send, val_recv)
    dens_copies = inner_copies(dens_own, lambda q: dens_in.at[q], dens_send, dens_recv)
    anc_copies = {
        s: pltpu.make_async_remote_copy(
            src_ref=anc.at[0],
            dst_ref=anc.at[s],
            send_sem=anc_send.at[s],
            recv_sem=anc_recv.at[s],
            device_id=outer_peer(s),
            device_id_type=MESH,
        )
        for s in outer_offsets
    }
    part_copies = {
        s: pltpu.make_async_remote_copy(
            src_ref=part_own.at[s],
            dst_ref=part_in.at[s],
            send_sem=part_send.at[s],
            recv_sem=part_recv.at[s],
            device_id=outer_peer(s, -1),
            device_id_type=MESH,
        )
        for s in outer_offsets
    }

    pl.semaphore_wait(barrier, (h - 1) + (g - 1))
    loads[0].wait()
    for q in inner_offsets:
        tgt_copies[q].start()
    loads[1].wait()
    for s in outer_offsets:
        anc_copies[s].start()
    for load in loads[2:]:
        load.wait()
    for q in inner_offsets:
        val_copies[q].start()

    dates, assets = vol.shape
    picked = lax.broadcasted_iota(jnp.int32, (dates, assets), 0) == date[0]
    vol_lanes = jnp.sum(jnp.where(picked, vol[...], 0.0), axis=0, keepdims=True)
    eye = lax.broadcasted_iota(jnp.int32, (assets, assets), 0) == lax.broadcasted_iota(
        jnp.int32, (assets, assets), 1
    )
    vol_row = jnp.sum(jnp.where(eye, vol_lanes, 0.0), axis=1, keepdims=True)
    scale = math.sqrt(math.log2(math.e)) / (vol_row * math.sqrt(step_years))
    drift = (rate_year - 0.5 * vol_row * vol_row) * step_years

    rows, columns = {}, {}
    outer_order = [0] + outer_offsets[::-1]
    near = [q for q in range(g) if q < low_count]
    far = [q for q in range(g) if q >= low_count]

    def block(s, q):
        exponent = jnp.dot(rows[s], columns[q], preferred_element_type=jnp.float32)
        weights = jnp.exp2(exponent)
        kmat[s, :, q * n : (q + 1) * n] = weights
        return jnp.sum(weights.reshape(n // 8, 8, n), axis=0)

    density = {q: jnp.zeros((8, n), jnp.float32) for q in range(g)}
    for part in [near] + [[q] for q in reversed(far)]:
        for q in part:
            if q:
                tgt_copies[q].wait_recv()
            columns[q] = target_stack(tgt[owner(q)] * scale)
        for s in outer_order:
            if s not in rows:
                if s:
                    anc_copies[s].wait_recv()
                rows[s] = jnp.transpose(anchor_stack((anc[s] + drift) * scale))
            for q in part:
                density[q] = density[q] + block(s, q)
        for q in part:
            dens_own[owner(q)] = jnp.sum(density[q], axis=0, keepdims=True)

    for q in inner_offsets:
        dens_copies[q].start()
    best = jnp.max(jnp.exp(anc[0]), axis=0, keepdims=True)
    for q in inner_offsets:
        val_copies[q].wait_recv()
    for q in inner_offsets:
        dens_copies[q].wait_recv()
    worth, inverse = {}, {}
    for q in range(g):
        total = dens_own[owner(q)]
        for p in inner_offsets:
            total = total + dens_in[p, owner(q)]
        inverse[q] = 1.0 / total
        worth[q] = val[owner(q)] / total

    for s in outer_order[::-1]:
        weighted = jnp.zeros((n, 128), jnp.float32)
        mass = jnp.zeros((n, 128), jnp.float32)
        for q in range(g):
            for c in range(0, n, 128):
                tile = kmat[s, :, q * n + c : q * n + c + 128]
                weighted = weighted + tile * worth[q][:, c : c + 128]
                mass = mass + tile * inverse[q][:, c : c + 128]
        part_own[s, 0:1, :] = jnp.sum(jnp.transpose(weighted), axis=0, keepdims=True)
        part_own[s, 1:2, :] = jnp.sum(jnp.transpose(mass), axis=0, keepdims=True)
        if s:
            part_copies[s].start()
    sums = part_own[0]
    for s in outer_offsets[::-1]:
        part_copies[s].wait_recv()
        sums = sums + part_in[s]
    weighted_ref[...] = sums[0]
    mass_ref[...] = sums[1]
    best_ref[...] = best.reshape(n)
    for copies in (anc_copies, tgt_copies, val_copies, dens_copies, part_copies):
        for copy in copies.values():
            copy.wait_send()


def body(count, current_states, next_states, next_values, vol_table, date_index, strike):
    assets, n = current_states.shape
    g = inner_size(count)
    h = count // g
    f32 = jnp.float32
    dma = pltpu.SemaphoreType.DMA
    row = pltpu.VMEM((n,), f32)
    w, m, p = pl.pallas_call(
        functools.partial(kernel, g, h),
        out_shape=(row, row, row),
        in_specs=[pl.BlockSpec(memory_space=pltpu.HBM)] * 5,
        out_specs=(pl.BlockSpec(memory_space=pltpu.VMEM),) * 3,
        scratch_shapes=[
            pltpu.VMEM((h, assets, n), f32),
            pltpu.VMEM((g, assets, n), f32),
            pltpu.VMEM((g, 1, n), f32),
            pltpu.VMEM(vol_table.shape, f32),
            pltpu.SMEM((1,), jnp.int32),
            pltpu.VMEM((h, n, g * n), f32),
            pltpu.VMEM((g, 1, n), f32),
            pltpu.VMEM((g, g, 1, n), f32),
            pltpu.VMEM((h, 2, n), f32),
            pltpu.VMEM((h, 2, n), f32),
            dma((5,)),
            dma((h,)),
            dma((h,)),
            dma((g,)),
            dma((g,)),
            dma((g,)),
            dma((g,)),
            dma((g,)),
            dma((g,)),
            dma((h,)),
            dma((h,)),
        ],
        compiler_params=pltpu.CompilerParams(collective_id=0, has_side_effects=True),
    )(current_states, next_states, next_values.reshape(1, n), vol_table, date_index)
    c = math.exp(-rate_year * step_years) * w / m
    return (c, jnp.maximum(jnp.maximum(p - strike[0], 0.0), c))


def solution(mesh):
    placed = (
        P(None, ("groups", "blk")),
        P(None, ("groups", "blk")),
        P(("groups", "blk")),
        P(),
        P(),
        P(),
    )
    return jax.shard_map(
        functools.partial(body, mesh.shape["blk"]),
        mesh=mesh,
        in_specs=placed,
        out_specs=(P(("groups", "blk")), P(("groups", "blk"))),
        check_vma=False,
    )
```
